32 devices in a mesh: interval: 4 (over x, core), rows: 8 (over z, y).
Axes of the slice: x: 2, y: 2, z: 4, core: 2. Of those that a mesh axis runs over, the one named last changes fastest.
Arguments:
- filtered: float32 [4, 64, 131072], P('interval', None, 'rows'), may hold values from -60 to 60, as said below
- potential: float32 [16, 64, 128], P('rows'), may hold values from 0.5 to 4
Outputs:
- basis: float32 [4, 64, 131072], P('interval', None, 'rows')
- ritz_matrix: float32 [4, 64, 64], P('interval')
- ritz_residual: float32 [4, 64, 131072], P('interval', None, 'rows')
The draws below stay inside these ranges and needn't reach their ends.
Inputs may be any that keep to these rules, and one draw needn't show every extreme that they name: `filtered`: the rows of each interval's block are linearly independent, and each interval's block shares a part with the block of the interval before it.
All inputs are finite; a program needn't handle non-finite values.
Results may differ from the reference program's by a relative error of at most 0.0003.
Values sent between devices are 32-bit elements; how exact they have to be, the bound alone decides.
A program may use at most 64 MiB of HBM per device.

```python
import math
import jax
import jax.numpy as jnp
from jax import lax

M = 64
GY = 64
GZ = 128
INTERVALS = 4
NX = 16
N = 131072


def draw_filtered(key, part):
    keys = jax.random.split(jax.random.fold_in(key, 11), 3)
    base = jax.random.normal(keys[0], (INTERVALS, M, N), jnp.float32)
    mixing = jax.random.normal(keys[1], (INTERVALS, M, M), jnp.float32) / math.sqrt(M)
    earlier = jnp.roll(base, 1, axis=0)
    mixed = base + 0.6 * jnp.einsum('imk,ikn->imn', mixing, earlier)
    scales = jnp.exp(jax.random.uniform(keys[2], (INTERVALS, M, 1), jnp.float32, 0.0, math.log(10.0)))
    plane = jnp.arange(N) // (GY * GZ)
    ramp = jnp.exp(math.log(3.0) * plane.astype(jnp.float32) / max(NX - 1, 1))
    return jnp.clip(mixed * scales * ramp[None, None, :], -60.0, 60.0).astype(jnp.float32)


def steps_of(own_key, shape, pieces, low, high):
    gain = 1.0
    for dim, blocks in pieces:
        draws = jax.random.uniform(jax.random.fold_in(jax.random.fold_in(own_key, 6), dim), (blocks,), jnp.float32, low / len(pieces), high / len(pieces))
        gain = gain * jnp.repeat(jnp.exp(draws), shape[dim] // blocks).reshape((-1,) + (1,) * (len(shape) - 1 - dim))
    return gain


def setup_inputs(seed: int = 0) -> dict:
    seeds = jax.random.split(jax.random.key(seed), 3)
    filtered = draw_filtered(jax.random.fold_in(seeds[2], 71), 0)
    potential = jnp.clip(jnp.exp(math.log(4.0) - 2.0794415 * jax.random.uniform(seeds[1], (NX, GY, GZ), jnp.float32) ** steps_of(seeds[1], (NX, GY, GZ), ((0, 8),), -0.2, 0.2)), 0.5, 4.0)
    return {"filtered": filtered, "potential": potential}


def inner(left, right):
    return lax.dot_general(left.astype(jnp.float32), right.astype(jnp.float32), (((1,), (1,)), ((), ())), precision=lax.Precision.HIGHEST, preferred_element_type=jnp.float32)

def apply_left(matrix, vectors):
    return jnp.dot(matrix.astype(jnp.float32), vectors.astype(jnp.float32), precision=lax.Precision.HIGHEST, preferred_element_type=jnp.float32)

def orthonormal(vectors):
    lower = jnp.linalg.cholesky(inner(vectors, vectors))
    return lax.linalg.triangular_solve(lower, vectors, left_side=True, lower=True)

def operate(field, potential):
    padded = jnp.pad(field, ((0, 0), (1, 1), (1, 1), (1, 1)))
    beside = padded[:, 2:, 1:-1, 1:-1] + padded[:, :-2, 1:-1, 1:-1]
    beside = beside + padded[:, 1:-1, 2:, 1:-1] + padded[:, 1:-1, :-2, 1:-1]
    beside = beside + padded[:, 1:-1, 1:-1, 2:] + padded[:, 1:-1, 1:-1, :-2]
    return (6.0 + potential) * field - beside

def reference(filtered, potential):
    count = filtered.shape[0]
    width = filtered.shape[1]
    owns = [orthonormal(filtered[index]) for index in range(count)]
    bases = []
    matrices = []
    residuals = []
    for index in range(count):
        own = owns[index]
        if index == 0:
            prior = jnp.zeros_like(own)
        else:
            prior = owns[index - 1]
        cross = inner(own, prior)
        reduced = own - apply_left(cross, prior)
        basis = orthonormal(reduced)
        image = operate(basis.reshape(width, NX, GY, GZ), potential).reshape(width, -1)
        ritz_matrix = inner(basis, image)
        residual = image - apply_left(ritz_matrix.T, basis)
        bases.append(basis)
        matrices.append(ritz_matrix)
        residuals.append(residual)
    return (jnp.stack(bases), jnp.stack(matrices), jnp.stack(residuals))
```

```python
import functools

import jax
import jax.numpy as jnp
from jax import lax
from jax.experimental import pallas as pl
from jax.experimental.pallas import tpu as pltpu
from jax.sharding import PartitionSpec as P

MESH = pl.DeviceIdType.MESH
CHUNKS = 8
EARLY = 4
F32 = jnp.float32


def split(x):
    high = x.astype(jnp.bfloat16)
    return high, (x - high.astype(F32)).astype(jnp.bfloat16)


def dot(left, right):
    return jnp.dot(left, right, preferred_element_type=F32)


def dot_nt(left, right):
    return lax.dot_general(left, right, (((1,), (1,)), ((), ())), preferred_element_type=F32)


def product(left, right):
    (lh, ll), (rh, rl) = left, split(right)
    return dot(lh, rh) + (dot(lh, rl) + dot(ll, rh))


def kernel(
    sizes, x_hbm, pot_ref, basis_hbm, ritz_ref, resid_hbm,
    x_ext, p_ext, b_ext, image, sums, gathered, system, weights,
    load_sem, store_sems, own_send, own_recv, halo_send, halo_recv,
    relay_send, relay_recv, sum_send, sum_recv,
):
    parts, intervals, width, plane, line, local = sizes
    tile = plane // CHUNKS
    tiles = local // tile
    own_tile = local // CHUNKS
    me = lax.axis_index("rows")
    interval = lax.axis_index("interval")
    has_before, has_after = me > 0, me < parts - 1
    has_prior, has_next = interval > 0, interval < intervals - 1
    two = 2 * width

    def peer(distance):
        return lax.rem(me + distance, parts)

    barrier = pltpu.get_barrier_semaphore()
    for distance in range(1, parts):
        pl.semaphore_signal(barrier, inc=1, device_id={"rows": peer(distance)}, device_id_type=MESH)

    @pl.when(has_prior)
    def _():
        pl.semaphore_signal(barrier, inc=1, device_id={"interval": interval - 1}, device_id_type=MESH)

    @pl.when(has_next)
    def _():
        pl.semaphore_signal(barrier, inc=1, device_id={"interval": interval + 1}, device_id_type=MESH)

    load = pltpu.make_async_copy(x_hbm, x_ext.at[:, pl.ds(plane, local)], load_sem)
    load.start()
    expected = parts - 1 + jnp.where(has_prior, 1, 0) + jnp.where(has_next, 1, 0)
    pl.semaphore_wait(barrier, expected)

    def own_copy(c):
        return pltpu.make_async_remote_copy(
            x_hbm.at[:, pl.ds(c * own_tile, own_tile)],
            p_ext.at[:, pl.ds(plane + c * own_tile, own_tile)],
            own_send.at[c], own_recv.at[c],
            device_id={"interval": interval + 1}, device_id_type=MESH,
        )

    def halo_copy(side, c):
        start = local - plane if side == 0 else 0
        land = 0 if side == 0 else plane + local
        to = me + 1 if side == 0 else me - 1
        return pltpu.make_async_remote_copy(
            x_hbm.at[:, pl.ds(start + c * tile, tile)],
            x_ext.at[:, pl.ds(land + c * tile, tile)],
            halo_send.at[side, c], halo_recv.at[side, c],
            device_id={"rows": to}, device_id_type=MESH,
        )

    def relay_copy(side, c):
        land = 0 if side == 0 else plane + local
        area = pl.ds(land + c * tile, tile)
        return pltpu.make_async_remote_copy(
            x_ext.at[:, area], p_ext.at[:, area],
            relay_send.at[side, c], relay_recv.at[side, c],
            device_id={"interval": interval + 1}, device_id_type=MESH,
        )

    sends = (has_after, has_before)
    receives = (has_before, has_after)

    def start_halo(c):
        for side in (0, 1):
            @pl.when(sends[side])
            def _():
                halo_copy(side, c).start()

    def relay(c):
        for side in (0, 1):
            @pl.when(receives[side])
            def _():
                halo_copy(side, c).wait_recv()

            @pl.when(receives[side] & has_next)
            def _():
                relay_copy(side, c).start()

    @pl.when(has_next)
    def _():
        for c in range(CHUNKS):
            own_copy(c).start()

    for c in range(EARLY):
        start_halo(c)

    def clear(ref, start, length):
        def step(t, carry):
            at = pl.multiple_of(start + t * tile, 128)
            ref[:, pl.ds(at, tile)] = jnp.zeros((width, tile), F32)
            return carry
        lax.fori_loop(0, length // tile, step, 0)

    for side, land in ((0, 0), (1, plane + local)):
        @pl.when(jnp.logical_not(receives[side]))
        def _():
            clear(x_ext, land, plane)

        @pl.when(jnp.logical_not(receives[side] & has_prior))
        def _():
            clear(p_ext, land, plane)

    @pl.when(jnp.logical_not(has_prior))
    def _():
        clear(p_ext, plane, local)

    load.wait()

    def add_gram(upper, lower):
        high, low = split(jnp.concatenate([upper, lower], axis=0))
        sums[0] += dot_nt(high, high)
        sums[1] += dot_nt(high, low)

    sums[...] = jnp.zeros_like(sums)
    inner_tiles = own_tile // tile
    for c in range(CHUNKS):
        @pl.when(has_prior)
        def _():
            own_copy(c).wait_recv()

        def gram_step(t, carry):
            at = pl.multiple_of(plane + c * own_tile + t * tile, 128)
            add_gram(p_ext[:, pl.ds(at, tile)], x_ext[:, pl.ds(at, tile)])
            return carry
        lax.fori_loop(0, inner_tiles, gram_step, 0)
        if c % 2 == 1 and c // 2 < EARLY:
            relay(c // 2)

    def sum_copy(turn, distance):
        return pltpu.make_async_remote_copy(
            gathered.at[turn, me], gathered.at[turn, me],
            sum_send.at[turn, distance], sum_recv.at[turn, me],
            device_id={"rows": peer(distance)}, device_id_type=MESH,
        )

    def arrival(turn, distance):
        sender = peer(distance)
        return pltpu.make_async_remote_copy(
            gathered.at[turn, sender], gathered.at[turn, sender],
            sum_send.at[turn, distance], sum_recv.at[turn, sender],
            device_id={"rows": sender}, device_id_type=MESH,
        )

    def start_sum(turn):
        gathered[turn, me] = sums[0] + (sums[1] + sums[1].T)
        for distance in range(1, parts):
            sum_copy(turn, distance).start()

    def finish_sum(turn):
        for distance in range(1, parts):
            arrival(turn, distance).wait_recv()
        total = gathered[turn, 0]
        for sender in range(1, parts):
            total = total + gathered[turn, sender]
        return total

    start_sum(0)
    for c in range(EARLY, CHUNKS):
        start_halo(c)
    gram = finish_sum(0)

    rows_at = lax.broadcasted_iota(jnp.int32, (two, two), 0)
    cols_at = lax.broadcasted_iota(jnp.int32, (two, two), 1)
    unit = jnp.where(rows_at == cols_at, 1.0, 0.0).astype(F32)
    lone = jnp.where(interval == 0, 1.0, 0.0).astype(F32)
    system[:, :two] = gram + lone * jnp.where(rows_at < width, unit, 0.0)
    system[:, two:] = unit

    def eliminate(k, carry):
        whole = system[...]
        row = system[pl.ds(k, 1), :]
        lane = lax.broadcasted_iota(jnp.int32, (1, two), 1)
        at = lax.broadcasted_iota(jnp.int32, (two, 1), 0)
        pivot = jnp.sum(jnp.where(lane == k, row[:, :two], 0.0), axis=1, keepdims=True)
        column = jnp.sum(jnp.where(lane == k, whole[:, :two], 0.0), axis=1, keepdims=True)
        scale = lax.rsqrt(pivot)
        scaled = row * scale
        below = jnp.where(at > k, column * scale, 0.0)
        system[...] = jnp.where(at == k, scaled, whole - below * scaled)
        return carry

    relay(EARLY)
    lax.fori_loop(0, width, eliminate, 0)
    relay(EARLY + 1)
    lax.fori_loop(width, two, eliminate, 0)
    for c in range(EARLY + 2, CHUNKS - 1):
        relay(c)
    weights[...] = system[width:, two:]

    def basis_at(at, mixing):
        at = pl.multiple_of(at, 128)
        both = jnp.concatenate([p_ext[:, pl.ds(at, tile)], x_ext[:, pl.ds(at, tile)]], axis=0)
        b_ext[:, pl.ds(at, tile)] = product(mixing, both)

    def own_step(t, carry):
        basis_at(plane + t * tile, split(weights[...]))
        return carry
    lax.fori_loop(0, tiles, own_step, 0)

    basis_out = pltpu.make_async_copy(b_ext.at[:, pl.ds(plane, local)], basis_hbm, store_sems.at[0])
    basis_out.start()

    relay(CHUNKS - 1)
    for c in range(CHUNKS):
        for side in (0, 1):
            @pl.when(receives[side] & has_prior)
            def _():
                relay_copy(side, c).wait_recv()

        for side, land in ((0, 0), (1, plane + local)):
            basis_at(land + c * tile, split(weights[...]))

    sums[...] = jnp.zeros_like(sums)
    lane_at = lax.broadcasted_iota(jnp.int32, (1, tile), 1)
    depth_at = lax.rem(lane_at, line)

    def image_step(t, carry):
        at = t * tile
        here = plane + at
        def near(offset):
            return b_ext[:, pl.ds(pl.multiple_of(here + offset, 128), tile)]
        block = near(0)
        in_plane = lax.rem(at, plane) + lane_at
        beside = near(-plane) + near(plane)
        beside = beside + jnp.where(in_plane >= line, near(-line), 0.0)
        beside = beside + jnp.where(in_plane < plane - line, near(line), 0.0)
        beside = beside + jnp.where(depth_at > 0, pltpu.roll(block, 1, 1), 0.0)
        beside = beside + jnp.where(depth_at < line - 1, pltpu.roll(block, tile - 1, 1), 0.0)
        where = pl.ds(pl.multiple_of(at, 128), tile)
        value = (6.0 + pot_ref[:, where]) * block - beside
        image[:, where] = value
        add_gram(block, value)
        return carry
    lax.fori_loop(0, tiles, image_step, 0)

    start_sum(1)
    projected = finish_sum(1)
    ritz_ref[...] = projected[:width]
    weights[:, :width] = projected[width:, :width]

    def residual_step(t, carry):
        at = pl.multiple_of(t * tile, 128)
        block = b_ext[:, pl.ds(pl.multiple_of(plane + t * tile, 128), tile)]
        image[:, pl.ds(at, tile)] -= product(split(weights[:, :width]), block)
        return carry
    for half in range(2):
        lax.fori_loop(half * (tiles // 2), (half + 1) * (tiles // 2), residual_step, 0)
        area = pl.ds(half * (local // 2), local // 2)
        pltpu.make_async_copy(image.at[:, area], resid_hbm.at[:, area], store_sems.at[1 + half]).start()

    basis_out.wait()
    for half in range(2):
        area = pl.ds(half * (local // 2), local // 2)
        pltpu.make_async_copy(image.at[:, area], resid_hbm.at[:, area], store_sems.at[1 + half]).wait()

    @pl.when(has_next)
    def _():
        for c in range(CHUNKS):
            own_copy(c).wait_send()
    for c in range(CHUNKS):
        for side in (0, 1):
            @pl.when(sends[side])
            def _():
                halo_copy(side, c).wait_send()

            @pl.when(receives[side] & has_next)
            def _():
                relay_copy(side, c).wait_send()
    for turn in (0, 1):
        for distance in range(1, parts):
            sum_copy(turn, distance).wait_send()


def solution(mesh):
    parts, intervals = mesh.shape["rows"], mesh.shape["interval"]

    def body(filtered, potential):
        vectors = filtered[0]
        width, local = vectors.shape
        planes, lines, line = potential.shape
        plane = lines * line
        extended = local + 2 * plane
        sizes = (parts, intervals, width, plane, line, local)
        hbm = pl.BlockSpec(memory_space=pl.ANY)
        vmem = pl.BlockSpec(memory_space=pltpu.VMEM)
        dma = pltpu.SemaphoreType.DMA
        basis, ritz, residual = pl.pallas_call(
            functools.partial(kernel, sizes),
            name="slicing",
            out_shape=(
                jax.ShapeDtypeStruct((width, local), F32),
                jax.ShapeDtypeStruct((width, 2 * width), F32),
                jax.ShapeDtypeStruct((width, local), F32),
            ),
            in_specs=[hbm, vmem],
            out_specs=(hbm, vmem, hbm),
            scratch_shapes=[
                pltpu.VMEM((width, extended), F32),
                pltpu.VMEM((width, extended), F32),
                pltpu.VMEM((width, extended), F32),
                pltpu.VMEM((width, local), F32),
                pltpu.VMEM((2, 2 * width, 2 * width), F32),
                pltpu.VMEM((2, parts, 2 * width, 2 * width), F32),
                pltpu.VMEM((2 * width, 4 * width), F32),
                pltpu.VMEM((width, 2 * width), F32),
                dma, dma((3,)),
                dma((CHUNKS,)), dma((CHUNKS,)),
                dma((2, CHUNKS)), dma((2, CHUNKS)),
                dma((2, CHUNKS)), dma((2, CHUNKS)),
                dma((2, parts)), dma((2, parts)),
            ],
            compiler_params=pltpu.CompilerParams(
                collective_id=0, has_side_effects=True, vmem_limit_bytes=60 * 1024 * 1024
            ),
        )(vectors, potential.reshape(1, local))
        return (basis[None], ritz[None, :, width:], residual[None])

    return jax.shard_map(
        body,
        mesh=mesh,
        in_specs=(P("interval", None, "rows"), P("rows", None, None)),
        out_specs=(
            P("interval", None, "rows"),
            P("interval", None, None),
            P("interval", None, "rows"),
        ),
        check_vma=False,
    )
```

```python
import functools

import jax
import jax.numpy as jnp
from jax import lax
from jax.experimental import pallas as pl
from jax.experimental.pallas import tpu as pltpu
from jax.sharding import PartitionSpec as P

MESH = pl.DeviceIdType.MESH
CHUNKS = 8
EARLY = 5
F32 = jnp.float32


def split(x):
    high = x.astype(jnp.bfloat16)
    return high, (x - high.astype(F32)).astype(jnp.bfloat16)


def dot(left, right):
    return jnp.dot(left, right, preferred_element_type=F32)


def dot_nt(left, right):
    return lax.dot_general(left, right, (((1,), (1,)), ((), ())), preferred_element_type=F32)


def product(left, right):
    (lh, ll), (rh, rl) = left, split(right)
    return dot(lh, rh) + (dot(lh, rl) + dot(ll, rh))


def kernel(
    sizes, x_hbm, pot_ref, basis_hbm, ritz_ref, resid_hbm,
    x_ext, p_ext, b_ext, image, sums, gathered, system, weights,
    load_sem, store_sems, own_send, own_recv, halo_send, halo_recv,
    relay_send, relay_recv, sum_send, sum_recv,
):
    parts, intervals, width, plane, line, local = sizes
    tile = plane // CHUNKS
    tiles = local // tile
    own_tile = local // CHUNKS
    me = lax.axis_index("rows")
    interval = lax.axis_index("interval")
    has_before, has_after = me > 0, me < parts - 1
    has_prior, has_next = interval > 0, interval < intervals - 1
    two = 2 * width

    def peer(distance):
        return lax.rem(me + distance, parts)

    barrier = pltpu.get_barrier_semaphore()
    for distance in range(1, parts):
        pl.semaphore_signal(barrier, inc=1, device_id={"rows": peer(distance)}, device_id_type=MESH)

    @pl.when(has_prior)
    def _():
        pl.semaphore_signal(barrier, inc=1, device_id={"interval": interval - 1}, device_id_type=MESH)

    @pl.when(has_next)
    def _():
        pl.semaphore_signal(barrier, inc=1, device_id={"interval": interval + 1}, device_id_type=MESH)

    load = pltpu.make_async_copy(x_hbm, x_ext.at[:, pl.ds(plane, local)], load_sem)
    load.start()
    expected = parts - 1 + jnp.where(has_prior, 1, 0) + jnp.where(has_next, 1, 0)
    pl.semaphore_wait(barrier, expected)

    def own_copy(c):
        return pltpu.make_async_remote_copy(
            x_hbm.at[:, pl.ds(c * own_tile, own_tile)],
            p_ext.at[:, pl.ds(plane + c * own_tile, own_tile)],
            own_send.at[c], own_recv.at[c],
            device_id={"interval": interval + 1}, device_id_type=MESH,
        )

    def halo_copy(side, c):
        start = local - plane if side == 0 else 0
        land = 0 if side == 0 else plane + local
        to = me + 1 if side == 0 else me - 1
        return pltpu.make_async_remote_copy(
            x_hbm.at[:, pl.ds(pl.multiple_of(start + c * tile, 128), tile)],
            x_ext.at[:, pl.ds(pl.multiple_of(land + c * tile, 128), tile)],
            halo_send.at[side, c], halo_recv.at[side, c],
            device_id={"rows": to}, device_id_type=MESH,
        )

    def relay_copy(side, c):
        land = 0 if side == 0 else plane + local
        area = pl.ds(pl.multiple_of(land + c * tile, 128), tile)
        return pltpu.make_async_remote_copy(
            x_ext.at[:, area], p_ext.at[:, area],
            relay_send.at[side, c], relay_recv.at[side, c],
            device_id={"interval": interval + 1}, device_id_type=MESH,
        )

    sends = (has_after, has_before)
    receives = (has_before, has_after)

    def start_halo(c):
        for side in (0, 1):
            @pl.when(sends[side])
            def _():
                halo_copy(side, c).start()

    def relay(c):
        for side in (0, 1):
            @pl.when(receives[side])
            def _():
                halo_copy(side, c).wait_recv()

            @pl.when(receives[side] & has_next)
            def _():
                relay_copy(side, c).start()

    @pl.when(has_next)
    def _():
        for c in range(CHUNKS):
            own_copy(c).start()

    for c in range(EARLY):
        start_halo(c)

    def clear(ref, start, length):
        def step(t, carry):
            at = pl.multiple_of(start + t * tile, 128)
            ref[:, pl.ds(at, tile)] = jnp.zeros((width, tile), F32)
            return carry
        lax.fori_loop(0, length // tile, step, 0)

    for side, land in ((0, 0), (1, plane + local)):
        @pl.when(jnp.logical_not(receives[side]))
        def _():
            clear(x_ext, land, plane)

        @pl.when(jnp.logical_not(receives[side] & has_prior))
        def _():
            clear(p_ext, land, plane)

    @pl.when(jnp.logical_not(has_prior))
    def _():
        clear(p_ext, plane, local)

    load.wait()

    def add_gram(upper, lower):
        high, low = split(jnp.concatenate([upper, lower], axis=0))
        sums[0] += dot_nt(high, high)
        sums[1] += dot_nt(high, low)

    sums[...] = jnp.zeros_like(sums)
    inner_tiles = own_tile // tile
    for c in range(CHUNKS):
        @pl.when(has_prior)
        def _():
            own_copy(c).wait_recv()

        def gram_step(t, carry):
            at = pl.multiple_of(plane + c * own_tile + t * tile, 128)
            add_gram(p_ext[:, pl.ds(at, tile)], x_ext[:, pl.ds(at, tile)])
            return carry
        lax.fori_loop(0, inner_tiles, gram_step, 0)

    def sum_copy(turn, distance):
        return pltpu.make_async_remote_copy(
            gathered.at[turn, me], gathered.at[turn, me],
            sum_send.at[turn, distance], sum_recv.at[turn, me],
            device_id={"rows": peer(distance)}, device_id_type=MESH,
        )

    def arrival(turn, distance):
        sender = peer(distance)
        return pltpu.make_async_remote_copy(
            gathered.at[turn, sender], gathered.at[turn, sender],
            sum_send.at[turn, distance], sum_recv.at[turn, sender],
            device_id={"rows": sender}, device_id_type=MESH,
        )

    def start_sum(turn):
        gathered[turn, me] = sums[0] + (sums[1] + sums[1].T)
        for distance in range(1, parts):
            sum_copy(turn, distance).start()

    def finish_sum(turn):
        for distance in range(1, parts):
            arrival(turn, distance).wait_recv()
        total = gathered[turn, 0]
        for sender in range(1, parts):
            total = total + gathered[turn, sender]
        return total

    start_sum(0)
    start_halo(EARLY)
    for c in range(EARLY):
        relay(c)
    gram = finish_sum(0)

    rows_at = lax.broadcasted_iota(jnp.int32, (two, two), 0)
    cols_at = lax.broadcasted_iota(jnp.int32, (two, two), 1)
    unit = jnp.where(rows_at == cols_at, 1.0, 0.0).astype(F32)
    lone = jnp.where(interval == 0, 1.0, 0.0).astype(F32)
    system[:, :two] = gram + lone * jnp.where(rows_at < width, unit, 0.0)
    system[:, two:] = unit

    def eliminate(k, carry):
        whole = system[...]
        row = system[pl.ds(k, 1), :]
        lane = lax.broadcasted_iota(jnp.int32, (1, two), 1)
        at = lax.broadcasted_iota(jnp.int32, (two, 1), 0)
        pivot = jnp.sum(jnp.where(lane == k, row[:, :two], 0.0), axis=1, keepdims=True)
        column = jnp.sum(jnp.where(lane == k, whole[:, :two], 0.0), axis=1, keepdims=True)
        scale = lax.rsqrt(pivot)
        scaled = row * scale
        below = jnp.where(at > k, column * scale, 0.0)
        system[...] = jnp.where(at == k, scaled, whole - below * scaled)
        return carry

    lax.fori_loop(0, width // 2, eliminate, 0)
    start_halo(EARLY + 1)
    lax.fori_loop(width // 2, width + width // 2, eliminate, 0)
    start_halo(EARLY + 2)
    relay(EARLY)
    lax.fori_loop(width + width // 2, two, eliminate, 0)
    weights[...] = system[width:, two:]

    def basis_at(at, mixing):
        at = pl.multiple_of(at, 128)
        both = jnp.concatenate([p_ext[:, pl.ds(at, tile)], x_ext[:, pl.ds(at, tile)]], axis=0)
        b_ext[:, pl.ds(at, tile)] = product(mixing, both)

    def own_step(t, carry):
        basis_at(plane + t * tile, split(weights[...]))
        return carry
    lax.fori_loop(0, tiles, own_step, 0)

    basis_out = pltpu.make_async_copy(b_ext.at[:, pl.ds(plane, local)], basis_hbm, store_sems.at[0])
    basis_out.start()

    relay(EARLY + 1)
    sums[...] = jnp.zeros_like(sums)
    lane_at = lax.broadcasted_iota(jnp.int32, (1, tile), 1)
    depth_at = lax.rem(lane_at, line)

    def image_step(t, carry):
        at = t * tile
        here = plane + at
        def near(offset):
            return b_ext[:, pl.ds(pl.multiple_of(here + offset, 128), tile)]
        block = near(0)
        in_plane = lax.rem(at, plane) + lane_at
        beside = near(-plane) + near(plane)
        beside = beside + jnp.where(in_plane >= line, near(-line), 0.0)
        beside = beside + jnp.where(in_plane < plane - line, near(line), 0.0)
        beside = beside + jnp.where(depth_at > 0, pltpu.roll(block, 1, 1), 0.0)
        beside = beside + jnp.where(depth_at < line - 1, pltpu.roll(block, tile - 1, 1), 0.0)
        where = pl.ds(pl.multiple_of(at, 128), tile)
        value = (6.0 + pot_ref[:, where]) * block - beside
        image[:, where] = value
        add_gram(block, value)
        return carry

    def chunk_step(c, carry):
        for side, land in ((0, 0), (1, plane + local)):
            @pl.when(receives[side] & has_prior)
            def _():
                relay_copy(side, c).wait_recv()
            basis_at(land + c * tile, split(weights[...]))

        def plane_step(p, inner):
            return image_step(p * CHUNKS + c, inner)
        return lax.fori_loop(0, local // plane, plane_step, carry)

    lax.fori_loop(0, CHUNKS - 1, chunk_step, 0)
    relay(CHUNKS - 1)
    chunk_step(CHUNKS - 1, 0)

    start_sum(1)
    projected = finish_sum(1)
    ritz_ref[...] = projected[:width]
    weights[:, :width] = projected[width:, :width]

    def residual_step(t, carry):
        at = pl.multiple_of(t * tile, 128)
        block = b_ext[:, pl.ds(pl.multiple_of(plane + t * tile, 128), tile)]
        image[:, pl.ds(at, tile)] -= product(split(weights[:, :width]), block)
        return carry
    for half in range(2):
        lax.fori_loop(half * (tiles // 2), (half + 1) * (tiles // 2), residual_step, 0)
        area = pl.ds(half * (local // 2), local // 2)
        pltpu.make_async_copy(image.at[:, area], resid_hbm.at[:, area], store_sems.at[1 + half]).start()

    basis_out.wait()
    for half in range(2):
        area = pl.ds(half * (local // 2), local // 2)
        pltpu.make_async_copy(image.at[:, area], resid_hbm.at[:, area], store_sems.at[1 + half]).wait()

    @pl.when(has_next)
    def _():
        for c in range(CHUNKS):
            own_copy(c).wait_send()
    for c in range(CHUNKS):
        for side in (0, 1):
            @pl.when(sends[side])
            def _():
                halo_copy(side, c).wait_send()

            @pl.when(receives[side] & has_next)
            def _():
                relay_copy(side, c).wait_send()
    for turn in (0, 1):
        for distance in range(1, parts):
            sum_copy(turn, distance).wait_send()


def solution(mesh):
    parts, intervals = mesh.shape["rows"], mesh.shape["interval"]

    def body(filtered, potential):
        vectors = filtered[0]
        width, local = vectors.shape
        planes, lines, line = potential.shape
        plane = lines * line
        extended = local + 2 * plane
        sizes = (parts, intervals, width, plane, line, local)
        hbm = pl.BlockSpec(memory_space=pl.ANY)
        vmem = pl.BlockSpec(memory_space=pltpu.VMEM)
        dma = pltpu.SemaphoreType.DMA
        basis, ritz, residual = pl.pallas_call(
            functools.partial(kernel, sizes),
            name="slicing",
            out_shape=(
                jax.ShapeDtypeStruct((width, local), F32),
                jax.ShapeDtypeStruct((width, 2 * width), F32),
                jax.ShapeDtypeStruct((width, local), F32),
            ),
            in_specs=[hbm, vmem],
            out_specs=(hbm, vmem, hbm),
            scratch_shapes=[
                pltpu.VMEM((width, extended), F32),
                pltpu.VMEM((width, extended), F32),
                pltpu.VMEM((width, extended), F32),
                pltpu.VMEM((width, local), F32),
                pltpu.VMEM((2, 2 * width, 2 * width), F32),
                pltpu.VMEM((2, parts, 2 * width, 2 * width), F32),
                pltpu.VMEM((2 * width, 4 * width), F32),
                pltpu.VMEM((width, 2 * width), F32),
                dma, dma((3,)),
                dma((CHUNKS,)), dma((CHUNKS,)),
                dma((2, CHUNKS)), dma((2, CHUNKS)),
                dma((2, CHUNKS)), dma((2, CHUNKS)),
                dma((2, parts)), dma((2, parts)),
            ],
            compiler_params=pltpu.CompilerParams(
                collective_id=0, has_side_effects=True, vmem_limit_bytes=42 * 1024 * 1024
            ),
        )(vectors, potential.reshape(1, local))
        return (basis[None], ritz[None, :, width:], residual[None])

    return jax.shard_map(
        body,
        mesh=mesh,
        in_specs=(P("interval", None, "rows"), P("rows", None, None)),
        out_specs=(
            P("interval", None, "rows"),
            P("interval", None, None),
            P("interval", None, "rows"),
        ),
        check_vma=False,
    )
```

```python
import functools

import jax
import jax.numpy as jnp
from jax import lax
from jax.experimental import pallas as pl
from jax.experimental.pallas import tpu as pltpu
from jax.sharding import PartitionSpec as P

MESH = pl.DeviceIdType.MESH
CHUNKS = 8
EARLY = 4
F32 = jnp.float32


def split(x):
    high = x.astype(jnp.bfloat16)
    return high, (x - high.astype(F32)).astype(jnp.bfloat16)


def dot(left, right):
    return jnp.dot(left, right, preferred_element_type=F32)


def dot_nt(left, right):
    return lax.dot_general(left, right, (((1,), (1,)), ((), ())), preferred_element_type=F32)


def product(left, right):
    (lh, ll), (rh, rl) = left, split(right)
    return dot(lh, rh) + (dot(lh, rl) + dot(ll, rh))


def kernel(
    sizes, x_hbm, pot_ref, basis_hbm, ritz_ref, resid_hbm,
    x_ext, p_ext, b_ext, image, sums, gathered, system, weights,
    load_sem, store_sems, own_send, own_recv, halo_send, halo_recv,
    relay_send, relay_recv, sum_send, sum_recv,
):
    parts, intervals, width, plane, line, local = sizes
    tile = plane // CHUNKS
    tiles = local // tile
    own_tile = local // CHUNKS
    me = lax.axis_index("rows")
    interval = lax.axis_index("interval")
    has_before, has_after = me > 0, me < parts - 1
    has_prior, has_next = interval > 0, interval < intervals - 1
    two = 2 * width

    def peer(distance):
        return lax.rem(me + distance, parts)

    barrier = pltpu.get_barrier_semaphore()
    for distance in range(1, parts):
        pl.semaphore_signal(barrier, inc=1, device_id={"rows": peer(distance)}, device_id_type=MESH)

    @pl.when(has_prior)
    def _():
        pl.semaphore_signal(barrier, inc=1, device_id={"interval": interval - 1}, device_id_type=MESH)

    @pl.when(has_next)
    def _():
        pl.semaphore_signal(barrier, inc=1, device_id={"interval": interval + 1}, device_id_type=MESH)

    load = pltpu.make_async_copy(x_hbm, x_ext.at[:, pl.ds(plane, local)], load_sem)
    load.start()
    expected = parts - 1 + jnp.where(has_prior, 1, 0) + jnp.where(has_next, 1, 0)
    pl.semaphore_wait(barrier, expected)

    def own_copy(c):
        return pltpu.make_async_remote_copy(
            x_hbm.at[:, pl.ds(c * own_tile, own_tile)],
            p_ext.at[:, pl.ds(plane + c * own_tile, own_tile)],
            own_send.at[c], own_recv.at[c],
            device_id={"interval": interval + 1}, device_id_type=MESH,
        )

    def halo_copy(side, c):
        start = local - plane if side == 0 else 0
        land = 0 if side == 0 else plane + local
        to = me + 1 if side == 0 else me - 1
        return pltpu.make_async_remote_copy(
            x_hbm.at[:, pl.ds(pl.multiple_of(start + c * tile, 128), tile)],
            x_ext.at[:, pl.ds(pl.multiple_of(land + c * tile, 128), tile)],
            halo_send.at[side, c], halo_recv.at[side, c],
            device_id={"rows": to}, device_id_type=MESH,
        )

    def relay_copy(side, c):
        land = 0 if side == 0 else plane + local
        area = pl.ds(pl.multiple_of(land + c * tile, 128), tile)
        return pltpu.make_async_remote_copy(
            x_ext.at[:, area], p_ext.at[:, area],
            relay_send.at[side, c], relay_recv.at[side, c],
            device_id={"interval": interval + 1}, device_id_type=MESH,
        )

    sends = (has_after, has_before)
    receives = (has_before, has_after)

    def start_halo(c):
        for side in (0, 1):
            @pl.when(sends[side])
            def _():
                halo_copy(side, c).start()

    def relay(c):
        for side in (0, 1):
            @pl.when(receives[side])
            def _():
                halo_copy(side, c).wait_recv()

            @pl.when(receives[side] & has_next)
            def _():
                relay_copy(side, c).start()

    @pl.when(has_next)
    def _():
        for c in range(CHUNKS):
            own_copy(c).start()

    for c in range(EARLY):
        start_halo(c)

    def clear(ref, start, length):
        def step(t, carry):
            at = pl.multiple_of(start + t * tile, 128)
            ref[:, pl.ds(at, tile)] = jnp.zeros((width, tile), F32)
            return carry
        lax.fori_loop(0, length // tile, step, 0)

    for side, land in ((0, 0), (1, plane + local)):
        @pl.when(jnp.logical_not(receives[side]))
        def _():
            clear(x_ext, land, plane)

        @pl.when(jnp.logical_not(receives[side] & has_prior))
        def _():
            clear(p_ext, land, plane)

    @pl.when(jnp.logical_not(has_prior))
    def _():
        clear(p_ext, plane, local)

    load.wait()

    def add_gram(upper, lower):
        high, low = split(jnp.concatenate([upper, lower], axis=0))
        sums[0] += dot_nt(high, high)
        sums[1] += dot_nt(high, low)

    sums[...] = jnp.zeros_like(sums)
    inner_tiles = own_tile // tile
    for c in range(CHUNKS):
        @pl.when(has_prior)
        def _():
            own_copy(c).wait_recv()

        def gram_step(t, carry):
            at = pl.multiple_of(plane + c * own_tile + t * tile, 128)
            add_gram(p_ext[:, pl.ds(at, tile)], x_ext[:, pl.ds(at, tile)])
            return carry
        lax.fori_loop(0, inner_tiles, gram_step, 0)

    def sum_copy(turn, distance):
        return pltpu.make_async_remote_copy(
            gathered.at[turn, me], gathered.at[turn, me],
            sum_send.at[turn, distance], sum_recv.at[turn, me],
            device_id={"rows": peer(distance)}, device_id_type=MESH,
        )

    def arrival(turn, distance):
        sender = peer(distance)
        return pltpu.make_async_remote_copy(
            gathered.at[turn, sender], gathered.at[turn, sender],
            sum_send.at[turn, distance], sum_recv.at[turn, sender],
            device_id={"rows": sender}, device_id_type=MESH,
        )

    def start_sum(turn):
        gathered[turn, me] = sums[0] + (sums[1] + sums[1].T)
        for distance in range(1, parts):
            sum_copy(turn, distance).start()

    def finish_sum(turn):
        for distance in range(1, parts):
            arrival(turn, distance).wait_recv()
        total = gathered[turn, 0]
        for sender in range(1, parts):
            total = total + gathered[turn, sender]
        return total

    start_sum(0)
    start_halo(EARLY)
    start_halo(EARLY + 1)
    for c in range(EARLY):
        relay(c)
    gram = finish_sum(0)

    rows_at = lax.broadcasted_iota(jnp.int32, (two, two), 0)
    cols_at = lax.broadcasted_iota(jnp.int32, (two, two), 1)
    unit = jnp.where(rows_at == cols_at, 1.0, 0.0).astype(F32)
    lone = jnp.where(interval == 0, 1.0, 0.0).astype(F32)
    system[:, :two] = gram + lone * jnp.where(rows_at < width, unit, 0.0)
    system[:, two:] = unit

    def eliminate(k, carry):
        whole = system[...]
        row = system[pl.ds(k, 1), :]
        lane = lax.broadcasted_iota(jnp.int32, (1, two), 1)
        at = lax.broadcasted_iota(jnp.int32, (two, 1), 0)
        pivot = jnp.sum(jnp.where(lane == k, row[:, :two], 0.0), axis=1, keepdims=True)
        column = jnp.sum(jnp.where(lane == k, whole[:, :two], 0.0), axis=1, keepdims=True)
        scale = lax.rsqrt(pivot)
        scaled = row * scale
        below = jnp.where(at > k, column * scale, 0.0)
        system[...] = jnp.where(at == k, scaled, whole - below * scaled)
        return carry

    lax.fori_loop(0, width // 2, eliminate, 0)
    start_halo(EARLY + 2)
    lax.fori_loop(width // 2, width + width // 2, eliminate, 0)
    start_halo(EARLY + 3)
    lax.fori_loop(width + width // 2, two, eliminate, 0)
    weights[...] = system[width:, two:]

    def basis_at(at, mixing):
        at = pl.multiple_of(at, 128)
        both = jnp.concatenate([p_ext[:, pl.ds(at, tile)], x_ext[:, pl.ds(at, tile)]], axis=0)
        b_ext[:, pl.ds(at, tile)] = product(mixing, both)

    def own_step(t, carry):
        basis_at(plane + t * tile, split(weights[...]))
        return carry
    lax.fori_loop(0, tiles, own_step, 0)

    basis_out = pltpu.make_async_copy(b_ext.at[:, pl.ds(plane, local)], basis_hbm, store_sems.at[0])
    basis_out.start()

    relay(EARLY)
    relay(EARLY + 1)
    sums[...] = jnp.zeros_like(sums)
    lane_at = lax.broadcasted_iota(jnp.int32, (1, tile), 1)
    depth_at = lax.rem(lane_at, line)

    def image_step(t, carry):
        at = t * tile
        here = plane + at
        def near(offset):
            return b_ext[:, pl.ds(pl.multiple_of(here + offset, 128), tile)]
        block = near(0)
        in_plane = lax.rem(at, plane) + lane_at
        beside = near(-plane) + near(plane)
        beside = beside + jnp.where(in_plane >= line, near(-line), 0.0)
        beside = beside + jnp.where(in_plane < plane - line, near(line), 0.0)
        beside = beside + jnp.where(depth_at > 0, pltpu.roll(block, 1, 1), 0.0)
        beside = beside + jnp.where(depth_at < line - 1, pltpu.roll(block, tile - 1, 1), 0.0)
        where = pl.ds(pl.multiple_of(at, 128), tile)
        value = (6.0 + pot_ref[:, where]) * block - beside
        image[:, where] = value
        add_gram(block, value)
        return carry

    def chunk_step(c, carry):
        for side, land in ((0, 0), (1, plane + local)):
            @pl.when(receives[side] & has_prior)
            def _():
                relay_copy(side, c).wait_recv()
            basis_at(land + c * tile, split(weights[...]))

        def plane_step(p, inner):
            return image_step(p * CHUNKS + c, inner)
        return lax.fori_loop(0, local // plane, plane_step, carry)

    lax.fori_loop(0, EARLY, chunk_step, 0)
    relay(EARLY + 2)
    lax.fori_loop(EARLY, EARLY + 2, chunk_step, 0)
    relay(CHUNKS - 1)
    lax.fori_loop(EARLY + 2, CHUNKS, chunk_step, 0)

    start_sum(1)
    projected = finish_sum(1)
    ritz_ref[...] = projected[:width]
    weights[:, :width] = projected[width:, :width]

    def residual_step(t, carry):
        at = pl.multiple_of(t * tile, 128)
        block = b_ext[:, pl.ds(pl.multiple_of(plane + t * tile, 128), tile)]
        image[:, pl.ds(at, tile)] -= product(split(weights[:, :width]), block)
        return carry
    for half in range(2):
        lax.fori_loop(half * (tiles // 2), (half + 1) * (tiles // 2), residual_step, 0)
        area = pl.ds(half * (local // 2), local // 2)
        pltpu.make_async_copy(image.at[:, area], resid_hbm.at[:, area], store_sems.at[1 + half]).start()

    basis_out.wait()
    for half in range(2):
        area = pl.ds(half * (local // 2), local // 2)
        pltpu.make_async_copy(image.at[:, area], resid_hbm.at[:, area], store_sems.at[1 + half]).wait()

    @pl.when(has_next)
    def _():
        for c in range(CHUNKS):
            own_copy(c).wait_send()
    for c in range(CHUNKS):
        for side in (0, 1):
            @pl.when(sends[side])
            def _():
                halo_copy(side, c).wait_send()

            @pl.when(receives[side] & has_next)
            def _():
                relay_copy(side, c).wait_send()
    for turn in (0, 1):
        for distance in range(1, parts):
            sum_copy(turn, distance).wait_send()


def solution(mesh):
    parts, intervals = mesh.shape["rows"], mesh.shape["interval"]

    def body(filtered, potential):
        vectors = filtered[0]
        width, local = vectors.shape
        planes, lines, line = potential.shape
        plane = lines * line
        extended = local + 2 * plane
        sizes = (parts, intervals, width, plane, line, local)
        hbm = pl.BlockSpec(memory_space=pl.ANY)
        vmem = pl.BlockSpec(memory_space=pltpu.VMEM)
        dma = pltpu.SemaphoreType.DMA
        basis, ritz, residual = pl.pallas_call(
            functools.partial(kernel, sizes),
            name="slicing",
            out_shape=(
                jax.ShapeDtypeStruct((width, local), F32),
                jax.ShapeDtypeStruct((width, 2 * width), F32),
                jax.ShapeDtypeStruct((width, local), F32),
            ),
            in_specs=[hbm, vmem],
            out_specs=(hbm, vmem, hbm),
            scratch_shapes=[
                pltpu.VMEM((width, extended), F32),
                pltpu.VMEM((width, extended), F32),
                pltpu.VMEM((width, extended), F32),
                pltpu.VMEM((width, local), F32),
                pltpu.VMEM((2, 2 * width, 2 * width), F32),
                pltpu.VMEM((2, parts, 2 * width, 2 * width), F32),
                pltpu.VMEM((2 * width, 4 * width), F32),
                pltpu.VMEM((width, 2 * width), F32),
                dma, dma((3,)),
                dma((CHUNKS,)), dma((CHUNKS,)),
                dma((2, CHUNKS)), dma((2, CHUNKS)),
                dma((2, CHUNKS)), dma((2, CHUNKS)),
                dma((2, parts)), dma((2, parts)),
            ],
            compiler_params=pltpu.CompilerParams(
                collective_id=0, has_side_effects=True, vmem_limit_bytes=42 * 1024 * 1024
            ),
        )(vectors, potential.reshape(1, local))
        return (basis[None], ritz[None, :, width:], residual[None])

    return jax.shard_map(
        body,
        mesh=mesh,
        in_specs=(P("interval", None, "rows"), P("rows", None, None)),
        out_specs=(
            P("interval", None, "rows"),
            P("interval", None, None),
            P("interval", None, "rows"),
        ),
        check_vma=False,
    )
```

```python
import functools

import jax
import jax.numpy as jnp
from jax import lax
from jax.experimental import pallas as pl
from jax.experimental.pallas import tpu as pltpu
from jax.sharding import PartitionSpec as P

MESH = pl.DeviceIdType.MESH
CHUNKS = 8
EARLY = 4
F32 = jnp.float32


def split(x):
    high = x.astype(jnp.bfloat16)
    return high, (x - high.astype(F32)).astype(jnp.bfloat16)


def dot(left, right):
    return jnp.dot(left, right, preferred_element_type=F32)


def dot_nt(left, right):
    return lax.dot_general(left, right, (((1,), (1,)), ((), ())), preferred_element_type=F32)


def product(left, right):
    (lh, ll), (rh, rl) = left, split(right)
    return dot(lh, rh) + (dot(lh, rl) + dot(ll, rh))


def kernel(
    sizes, x_hbm, pot_ref, basis_hbm, ritz_ref, resid_hbm,
    x_ext, p_ext, b_ext, image, sums, gathered, system, weights,
    load_sem, store_sems, own_send, own_recv, halo_send, halo_recv,
    relay_send, relay_recv, sum_send, sum_recv,
):
    parts, intervals, width, plane, line, local = sizes
    tile = plane // CHUNKS
    tiles = local // tile
    own_tile = local // CHUNKS
    me = lax.axis_index("rows")
    interval = lax.axis_index("interval")
    has_before, has_after = me > 0, me < parts - 1
    has_prior, has_next = interval > 0, interval < intervals - 1
    two = 2 * width

    def peer(distance):
        return lax.rem(me + distance, parts)

    barrier = pltpu.get_barrier_semaphore()
    for distance in range(1, parts):
        pl.semaphore_signal(barrier, inc=1, device_id={"rows": peer(distance)}, device_id_type=MESH)

    @pl.when(has_prior)
    def _():
        pl.semaphore_signal(barrier, inc=1, device_id={"interval": interval - 1}, device_id_type=MESH)

    @pl.when(has_next)
    def _():
        pl.semaphore_signal(barrier, inc=1, device_id={"interval": interval + 1}, device_id_type=MESH)

    load = pltpu.make_async_copy(x_hbm, x_ext.at[:, pl.ds(plane, local)], load_sem)
    load.start()
    expected = parts - 1 + jnp.where(has_prior, 1, 0) + jnp.where(has_next, 1, 0)
    pl.semaphore_wait(barrier, expected)

    def own_copy(c):
        return pltpu.make_async_remote_copy(
            x_hbm.at[:, pl.ds(c * own_tile, own_tile)],
            p_ext.at[:, pl.ds(plane + c * own_tile, own_tile)],
            own_send.at[c], own_recv.at[c],
            device_id={"interval": interval + 1}, device_id_type=MESH,
        )

    def halo_copy(side, c):
        start = local - plane if side == 0 else 0
        land = 0 if side == 0 else plane + local
        to = me + 1 if side == 0 else me - 1
        return pltpu.make_async_remote_copy(
            x_hbm.at[:, pl.ds(pl.multiple_of(start + c * tile, 128), tile)],
            x_ext.at[:, pl.ds(pl.multiple_of(land + c * tile, 128), tile)],
            halo_send.at[side, c], halo_recv.at[side, c],
            device_id={"rows": to}, device_id_type=MESH,
        )

    def relay_copy(side, c):
        land = 0 if side == 0 else plane + local
        area = pl.ds(pl.multiple_of(land + c * tile, 128), tile)
        return pltpu.make_async_remote_copy(
            x_ext.at[:, area], p_ext.at[:, area],
            relay_send.at[side, c], relay_recv.at[side, c],
            device_id={"interval": interval + 1}, device_id_type=MESH,
        )

    sends = (has_after, has_before)
    receives = (has_before, has_after)

    def start_halo(c):
        for side in (0, 1):
            @pl.when(sends[side])
            def _():
                halo_copy(side, c).start()

    def relay(c):
        for side in (0, 1):
            @pl.when(receives[side])
            def _():
                halo_copy(side, c).wait_recv()

            @pl.when(receives[side] & has_next)
            def _():
                relay_copy(side, c).start()

    @pl.when(has_next)
    def _():
        for c in range(CHUNKS):
            own_copy(c).start()

    for c in range(EARLY):
        start_halo(c)

    def clear(ref, start, length):
        def step(t, carry):
            at = pl.multiple_of(start + t * tile, 128)
            ref[:, pl.ds(at, tile)] = jnp.zeros((width, tile), F32)
            return carry
        lax.fori_loop(0, length // tile, step, 0)

    for side, land in ((0, 0), (1, plane + local)):
        @pl.when(jnp.logical_not(receives[side]))
        def _():
            clear(x_ext, land, plane)

        @pl.when(jnp.logical_not(receives[side] & has_prior))
        def _():
            clear(p_ext, land, plane)

    @pl.when(jnp.logical_not(has_prior))
    def _():
        clear(p_ext, plane, local)

    load.wait()

    def add_gram(upper, lower):
        high, low = split(jnp.concatenate([upper, lower], axis=0))
        sums[0] += dot_nt(high, high)
        sums[1] += dot_nt(high, low)

    sums[...] = jnp.zeros_like(sums)
    inner_tiles = own_tile // tile
    for c in range(CHUNKS):
        @pl.when(has_prior)
        def _():
            own_copy(c).wait_recv()

        def gram_step(t, carry):
            at = pl.multiple_of(plane + c * own_tile + t * tile, 128)
            add_gram(p_ext[:, pl.ds(at, tile)], x_ext[:, pl.ds(at, tile)])
            return carry
        lax.fori_loop(0, inner_tiles, gram_step, 0)

    def sum_copy(turn, distance):
        return pltpu.make_async_remote_copy(
            gathered.at[turn, me], gathered.at[turn, me],
            sum_send.at[turn, distance], sum_recv.at[turn, me],
            device_id={"rows": peer(distance)}, device_id_type=MESH,
        )

    def arrival(turn, distance):
        sender = peer(distance)
        return pltpu.make_async_remote_copy(
            gathered.at[turn, sender], gathered.at[turn, sender],
            sum_send.at[turn, distance], sum_recv.at[turn, sender],
            device_id={"rows": sender}, device_id_type=MESH,
        )

    def start_sum(turn):
        gathered[turn, me] = sums[0] + (sums[1] + sums[1].T)
        for distance in range(1, parts):
            sum_copy(turn, distance).start()

    def finish_sum(turn):
        for distance in range(1, parts):
            arrival(turn, distance).wait_recv()
        total = gathered[turn, 0]
        for sender in range(1, parts):
            total = total + gathered[turn, sender]
        return total

    start_sum(0)
    start_halo(EARLY)
    start_halo(EARLY + 1)
    for c in range(EARLY):
        relay(c)
    gram = finish_sum(0)

    rows_at = lax.broadcasted_iota(jnp.int32, (two, two), 0)
    cols_at = lax.broadcasted_iota(jnp.int32, (two, two), 1)
    unit = jnp.where(rows_at == cols_at, 1.0, 0.0).astype(F32)
    lone = jnp.where(interval == 0, 1.0, 0.0).astype(F32)
    system[:, :two] = gram + lone * jnp.where(rows_at < width, unit, 0.0)
    system[:, two:] = unit

    def eliminate(k, carry):
        whole = system[...]
        row = system[pl.ds(k, 1), :]
        lane = lax.broadcasted_iota(jnp.int32, (1, two), 1)
        at = lax.broadcasted_iota(jnp.int32, (two, 1), 0)
        pivot = jnp.sum(jnp.where(lane == k, row[:, :two], 0.0), axis=1, keepdims=True)
        column = jnp.sum(jnp.where(lane == k, whole[:, :two], 0.0), axis=1, keepdims=True)
        scale = lax.rsqrt(pivot)
        scaled = row * scale
        below = jnp.where(at > k, column * scale, 0.0)
        system[...] = jnp.where(at == k, scaled, whole - below * scaled)
        return carry

    lax.fori_loop(0, width // 2, eliminate, 0)
    start_halo(EARLY + 2)
    lax.fori_loop(width // 2, width + width // 2, eliminate, 0)
    start_halo(EARLY + 3)
    lax.fori_loop(width + width // 2, two, eliminate, 0)
    weights[...] = system[width:, two:]

    def basis_at(at, mixing):
        at = pl.multiple_of(at, 128)
        both = jnp.concatenate([p_ext[:, pl.ds(at, tile)], x_ext[:, pl.ds(at, tile)]], axis=0)
        b_ext[:, pl.ds(at, tile)] = product(mixing, both)

    def own_step(t, carry):
        basis_at(plane + t * tile, split(weights[...]))
        return carry
    lax.fori_loop(0, tiles, own_step, 0)

    basis_out = pltpu.make_async_copy(b_ext.at[:, pl.ds(plane, local)], basis_hbm, store_sems.at[0])
    basis_out.start()

    sums[...] = jnp.zeros_like(sums)
    lane_at = lax.broadcasted_iota(jnp.int32, (1, tile), 1)
    depth_at = lax.rem(lane_at, line)

    def image_step(t, carry):
        at = t * tile
        here = plane + at
        def near(offset):
            return b_ext[:, pl.ds(pl.multiple_of(here + offset, 128), tile)]
        block = near(0)
        in_plane = lax.rem(at, plane) + lane_at
        beside = near(-plane) + near(plane)
        beside = beside + jnp.where(in_plane >= line, near(-line), 0.0)
        beside = beside + jnp.where(in_plane < plane - line, near(line), 0.0)
        beside = beside + jnp.where(depth_at > 0, pltpu.roll(block, 1, 1), 0.0)
        beside = beside + jnp.where(depth_at < line - 1, pltpu.roll(block, tile - 1, 1), 0.0)
        where = pl.ds(pl.multiple_of(at, 128), tile)
        value = (6.0 + pot_ref[:, where]) * block - beside
        image[:, where] = value
        add_gram(block, value)
        return carry

    def chunk_step(c, carry):
        for side, land in ((0, 0), (1, plane + local)):
            @pl.when(receives[side] & has_prior)
            def _():
                relay_copy(side, c).wait_recv()
            basis_at(land + c * tile, split(weights[...]))

        def plane_step(p, inner):
            return image_step(p * CHUNKS + c, inner)
        return lax.fori_loop(0, local // plane, plane_step, carry)

    lax.fori_loop(0, EARLY, chunk_step, 0)
    for c in range(EARLY, CHUNKS - 1):
        relay(c)
    lax.fori_loop(EARLY, EARLY + 2, chunk_step, 0)
    relay(CHUNKS - 1)
    lax.fori_loop(EARLY + 2, CHUNKS, chunk_step, 0)

    start_sum(1)
    projected = finish_sum(1)
    ritz_ref[...] = projected[:width]
    weights[:, :width] = projected[width:, :width]

    def residual_step(t, carry):
        at = pl.multiple_of(t * tile, 128)
        block = b_ext[:, pl.ds(pl.multiple_of(plane + t * tile, 128), tile)]
        image[:, pl.ds(at, tile)] -= product(split(weights[:, :width]), block)
        return carry
    for half in range(2):
        lax.fori_loop(half * (tiles // 2), (half + 1) * (tiles // 2), residual_step, 0)
        area = pl.ds(half * (local // 2), local // 2)
        pltpu.make_async_copy(image.at[:, area], resid_hbm.at[:, area], store_sems.at[1 + half]).start()

    basis_out.wait()
    for half in range(2):
        area = pl.ds(half * (local // 2), local // 2)
        pltpu.make_async_copy(image.at[:, area], resid_hbm.at[:, area], store_sems.at[1 + half]).wait()

    @pl.when(has_next)
    def _():
        for c in range(CHUNKS):
            own_copy(c).wait_send()
    for c in range(CHUNKS):
        for side in (0, 1):
            @pl.when(sends[side])
            def _():
                halo_copy(side, c).wait_send()

            @pl.when(receives[side] & has_next)
            def _():
                relay_copy(side, c).wait_send()
    for turn in (0, 1):
        for distance in range(1, parts):
            sum_copy(turn, distance).wait_send()


def solution(mesh):
    parts, intervals = mesh.shape["rows"], mesh.shape["interval"]

    def body(filtered, potential):
        vectors = filtered[0]
        width, local = vectors.shape
        planes, lines, line = potential.shape
        plane = lines * line
        extended = local + 2 * plane
        sizes = (parts, intervals, width, plane, line, local)
        hbm = pl.BlockSpec(memory_space=pl.ANY)
        vmem = pl.BlockSpec(memory_space=pltpu.VMEM)
        dma = pltpu.SemaphoreType.DMA
        basis, ritz, residual = pl.pallas_call(
            functools.partial(kernel, sizes),
            name="slicing",
            out_shape=(
                jax.ShapeDtypeStruct((width, local), F32),
                jax.ShapeDtypeStruct((width, 2 * width), F32),
                jax.ShapeDtypeStruct((width, local), F32),
            ),
            in_specs=[hbm, vmem],
            out_specs=(hbm, vmem, hbm),
            scratch_shapes=[
                pltpu.VMEM((width, extended), F32),
                pltpu.VMEM((width, extended), F32),
                pltpu.VMEM((width, extended), F32),
                pltpu.VMEM((width, local), F32),
                pltpu.VMEM((2, 2 * width, 2 * width), F32),
                pltpu.VMEM((2, parts, 2 * width, 2 * width), F32),
                pltpu.VMEM((2 * width, 4 * width), F32),
                pltpu.VMEM((width, 2 * width), F32),
                dma, dma((3,)),
                dma((CHUNKS,)), dma((CHUNKS,)),
                dma((2, CHUNKS)), dma((2, CHUNKS)),
                dma((2, CHUNKS)), dma((2, CHUNKS)),
                dma((2, parts)), dma((2, parts)),
            ],
            compiler_params=pltpu.CompilerParams(
                collective_id=0, has_side_effects=True, vmem_limit_bytes=42 * 1024 * 1024
            ),
        )(vectors, potential.reshape(1, local))
        return (basis[None], ritz[None, :, width:], residual[None])

    return jax.shard_map(
        body,
        mesh=mesh,
        in_specs=(P("interval", None, "rows"), P("rows", None, None)),
        out_specs=(
            P("interval", None, "rows"),
            P("interval", None, None),
            P("interval", None, "rows"),
        ),
        check_vma=False,
    )
```
